32 devices in a mesh: seq: 16 (over z, x, core), head: 2 (over y).
Axes of the slice: x: 2, y: 2, z: 4, core: 2. Of those that a mesh axis runs over, the one named last changes fastest.
Arguments:
- queries: bfloat16 [8192, 512], P('seq', 'head'), may hold values from -60 to 60
- key_vectors: bfloat16 [8192, 512], P('seq', 'head'), may hold values from -6 to 6
- value_vectors: bfloat16 [8192, 512], P('seq', 'head'), may hold values from -6 to 6
- out_grad: bfloat16 [8192, 512], P('seq', 'head'), may hold values from -6 to 6
- out_weight: bfloat16 [512, 512], P('head'), may hold values from -0.25 to 0.25
- mid_keep: int32 [32, 48], P('seq'), may hold values 0 or 1
- frame_keep: int32 [32], P('seq'), may hold values from 0 to 1, as said below
Outputs:
- output: bfloat16 [8192, 512], P('seq', 'head')
- query_gradient: bfloat16 [8192, 512], P('seq', 'head')
- key_gradient: bfloat16 [8192, 512], P('seq', 'head')
- value_gradient: bfloat16 [8192, 512], P('seq', 'head')
- weight_grad: float32 [512, 512], P('head')
The draws below stay inside these ranges and needn't reach their ends.
Inputs may be any that keep to these rules, and one draw needn't show every extreme that they name: `frame_keep`: frame boundaries fall only inside shards: the first near block of every shard of 512 tokens holds 1.
All inputs are finite; a program needn't handle non-finite values. No bound on the sum of `mid_keep` on one device may be relied on, other than what follows from the above.
Results may differ from the reference program's by a relative error of at most 0.0057.
The reference program's roundings to bfloat16 on the way count: a program that leaves them out, or rounds other values in their place, can miss the bound.
Values may be sent and summed in bfloat16 or wider, within the bound.
No kernel may reach another device: no remote copies, remote signals or barrier semaphores. Data moves between devices by JAX's collectives and lax.ppermute only.
A program may use at most 64 MiB of HBM per device.

```python
import math
import jax
import jax.numpy as jnp
from jax import lax

HEADS = 8
HDIM = 64
FEAT = 512
TOK_DEV = 512
NEAR = 256
MIDG = 8
FARG = 128
REACH = 12
TOKENS = 8192
MWIDTH = 48


def shared_keys(key):
    key_table = jnp.clip(jax.random.normal(jax.random.fold_in(key, 104), (TOKENS, FEAT), jnp.float32), -6.0, 6.0)
    return key_table


def draw_key_vectors(key, part):
    return shared_keys(key).astype(jnp.bfloat16)


def draw_queries(key, part):
    result = jnp.clip(2.5 * jax.random.normal(jax.random.fold_in(key, 106), (TOKENS, FEAT), jnp.float32), -15.0, 15.0)
    return result.astype(jnp.bfloat16)


def draw_frame_keep(key, part):
    block_count = TOKENS // NEAR
    draws = jax.random.randint(jax.random.fold_in(key, 107), (block_count,), 0, 4, dtype=jnp.int32)
    block_ids = jnp.arange(block_count, dtype=jnp.int32)
    opening = block_ids % (TOK_DEV // NEAR) == 0
    return jnp.where(opening, 1, (draws > 0).astype(jnp.int32)).astype(jnp.int32)


def touch_ends(array, stream_key, least, largest):
    index_at = [jax.random.randint(jax.random.fold_in(stream_key, axis), (), 0, length) for axis, length in enumerate(array.shape)]
    longest = array.shape.index(max(array.shape))
    beside = index_at[:longest] + [(index_at[longest] + 1) % array.shape[longest]] + index_at[longest + 1:]
    return array.at[tuple(index_at)].set(least).at[tuple(beside)].set(largest)


def block_scale(key, dims, split, smallest, top_value):
    loudness = 1.0
    for position, blocks in split:
        steps = jax.random.uniform(jax.random.fold_in(jax.random.fold_in(key, 6), position), (blocks,), jnp.float32, smallest / len(split), top_value / len(split))
        loudness = loudness * jnp.repeat(jnp.exp(steps), dims[position] // blocks).reshape((-1,) + (1,) * (len(dims) - 1 - position))
    return loudness


def noise(key, extent, scale, most, cuts=(), kind=jnp.bfloat16):
    drawn = jax.random.normal(key, extent, jnp.float32) * scale
    if len(cuts) > 0:
        drawn = block_scale(key, extent, cuts, -0.22, 0.18) * drawn
    return jnp.clip(drawn, min=-most, max=most).astype(kind)


def setup_inputs(seed: int = 0) -> dict:
    keys = jax.random.split(jax.random.key(seed), 8)
    return {
        "queries": draw_queries(jax.random.fold_in(keys[7], 71), 0),
        "key_vectors": draw_key_vectors(jax.random.fold_in(keys[7], 71), 0),
        "value_vectors": noise(keys[2], (TOKENS, FEAT), 1.0, 6.0, ((0, 16), (1, 2))),
        "out_grad": noise(keys[3], (TOKENS, FEAT), 1.0, 6.0, ((0, 16), (1, 2))),
        "out_weight": noise(keys[4], (FEAT, FEAT), FEAT ** -0.5, 0.25, ((0, 2),)),
        "mid_keep": touch_ends((jax.random.randint(keys[5], (TOKENS // NEAR, MWIDTH), 0, 4) < 3).astype(jnp.int32), jax.random.fold_in(keys[5], 1), 0, 1),
        "frame_keep": draw_frame_keep(jax.random.fold_in(keys[7], 71), 0),
    }


def pooled(source, stride, rooted):
    total = source.astype(jnp.float32).reshape(-1, stride, source.shape[1]).sum(axis=1)
    divisor = math.sqrt(stride) if rooted else float(stride)
    return (total / divisor).astype(jnp.bfloat16)

def visibility(block_id, device_id, length, frame_flag, keep_row, coarse_count):
    query_pos = block_id * NEAR + jnp.arange(NEAR, dtype=jnp.int32)[:, None]
    near_pos = (block_id - 1) * NEAR + jnp.arange(2 * NEAR, dtype=jnp.int32)[None, :]
    near_seen = (near_pos <= query_pos) & (near_pos >= 0) & ((near_pos >= block_id * NEAR) | (frame_flag == 1))
    groups = length // MIDG
    starts = ((device_id - REACH) * groups + jnp.arange(REACH * groups, dtype=jnp.int32)) * MIDG
    kept = jnp.repeat(keep_row, FARG // MIDG) == 1
    middle_seen = (starts >= 0) & (starts + MIDG <= (block_id - 1) * NEAR) & kept
    far_seen = (jnp.arange(coarse_count, dtype=jnp.int32) + 1) * FARG <= (block_id - 1) * NEAR
    columns = jnp.concatenate([middle_seen, far_seen])
    return jnp.concatenate([near_seen, jnp.broadcast_to(columns[None, :], (NEAR, columns.shape[0]))], axis=1)

def attend(query_tile, key_tile, value_tile, visible, gradient_tile, scale_amount):
    query_float = query_tile.astype(jnp.float32)
    key_float = key_tile.astype(jnp.float32)
    value_float = value_tile.astype(jnp.float32)
    gradient_float = gradient_tile.astype(jnp.float32)
    logit_matrix = jnp.einsum('aos,ros->oar', query_float, key_float) * scale_amount
    logit_matrix = jnp.where(visible[None], logit_matrix, -1e+30)
    row_top = lax.optimization_barrier(jnp.max(logit_matrix, axis=2, keepdims=True))
    weights = jnp.exp(logit_matrix - row_top)
    shares = weights / lax.optimization_barrier(jnp.sum(weights, axis=2, keepdims=True))
    rounded_scores = shares.astype(jnp.bfloat16)
    mixed_result = jnp.einsum('svu,usc->vsc', rounded_scores.astype(jnp.float32), value_float).astype(jnp.bfloat16)
    shared_gradient = jnp.einsum('aos,ros->oar', gradient_float, value_float)
    centre = lax.optimization_barrier(jnp.sum(shares * shared_gradient, axis=2, keepdims=True))
    decay_slopes = (shares * (shared_gradient - centre)).astype(jnp.bfloat16).astype(jnp.float32)
    query_gradient = jnp.einsum('svu,usc->vsc', decay_slopes, key_float) * scale_amount
    key_gradient = jnp.einsum('equ,qeb->ueb', decay_slopes, query_float) * scale_amount
    value_gradient = jnp.einsum('equ,qeb->ueb', rounded_scores.astype(jnp.float32), gradient_float)
    return (mixed_result, query_gradient, key_gradient, value_gradient)

def slab(source, start, size):
    return lax.dynamic_slice_in_dim(source, start, size, 0)

def shaped(block_rows):
    return block_rows.reshape(block_rows.shape[0], HEADS, HDIM)

def reference(queries, key_vectors, value_vectors, out_grad, out_weight, mid_keep, frame_keep):
    scale_amount = HDIM ** (-0.5)
    device_blocks = TOK_DEV // NEAR
    groups = TOK_DEV // MIDG
    window_rows = REACH * groups
    coarse_count = TOKENS // FARG
    mixed_grad = jnp.dot(out_grad, out_weight.T, preferred_element_type=jnp.float32).astype(jnp.bfloat16)
    middle_keys = pooled(key_vectors, MIDG, True)
    middle_values = pooled(value_vectors, MIDG, False)
    coarse_keys = pooled(key_vectors, FARG, True)
    coarse_values = pooled(value_vectors, FARG, False)
    near_keys = jnp.concatenate([jnp.zeros((NEAR, FEAT), jnp.bfloat16), key_vectors], axis=0)
    near_values = jnp.concatenate([jnp.zeros((NEAR, FEAT), jnp.bfloat16), value_vectors], axis=0)
    front = jnp.zeros((REACH * groups, FEAT), jnp.bfloat16)
    padded_keys = jnp.concatenate([front, middle_keys], axis=0)
    padded_values = jnp.concatenate([front, middle_values], axis=0)

    def visit(carry, block_id):
        near_kg, near_vg, middle_kg, middle_vg, coarse_kg, coarse_vg = carry
        device_id = block_id // device_blocks
        head_row = block_id * NEAR
        window_row = device_id * groups
        key_tile = jnp.concatenate([slab(near_keys, head_row, 2 * NEAR), slab(padded_keys, window_row, window_rows), coarse_keys], axis=0)
        value_tile = jnp.concatenate([slab(near_values, head_row, 2 * NEAR), slab(padded_values, window_row, window_rows), coarse_values], axis=0)
        visible = visibility(block_id, device_id, TOK_DEV, frame_keep[block_id], mid_keep[block_id], coarse_count)
        mixed_result, query_part, key_part, value_part = attend(shaped(slab(queries, head_row, NEAR)), shaped(key_tile), shaped(value_tile), visible, shaped(slab(mixed_grad, head_row, NEAR)), scale_amount)
        key_part = key_part.reshape(-1, FEAT)
        value_part = value_part.reshape(-1, FEAT)
        near_kg = lax.dynamic_update_slice_in_dim(near_kg, slab(near_kg, head_row, 2 * NEAR) + key_part[:2 * NEAR], head_row, 0)
        near_vg = lax.dynamic_update_slice_in_dim(near_vg, slab(near_vg, head_row, 2 * NEAR) + value_part[:2 * NEAR], head_row, 0)
        middle_kg = lax.dynamic_update_slice_in_dim(middle_kg, slab(middle_kg, window_row, window_rows) + key_part[2 * NEAR:2 * NEAR + window_rows], window_row, 0)
        middle_vg = lax.dynamic_update_slice_in_dim(middle_vg, slab(middle_vg, window_row, window_rows) + value_part[2 * NEAR:2 * NEAR + window_rows], window_row, 0)
        coarse_kg = coarse_kg + key_part[2 * NEAR + window_rows:]
        coarse_vg = coarse_vg + value_part[2 * NEAR + window_rows:]
        return ((near_kg, near_vg, middle_kg, middle_vg, coarse_kg, coarse_vg), (mixed_result.reshape(NEAR, FEAT), query_part.reshape(NEAR, FEAT)))
    start_state = (jnp.zeros((NEAR + TOKENS, FEAT), jnp.float32), jnp.zeros((NEAR + TOKENS, FEAT), jnp.float32), jnp.zeros((REACH * groups + TOKENS // MIDG, FEAT), jnp.float32), jnp.zeros((REACH * groups + TOKENS // MIDG, FEAT), jnp.float32), jnp.zeros((coarse_count, FEAT), jnp.float32), jnp.zeros((coarse_count, FEAT), jnp.float32))
    final_state, stacked = lax.scan(visit, start_state, jnp.arange(TOKENS // NEAR, dtype=jnp.int32))
    near_kg, near_vg, middle_kg, middle_vg, coarse_kg, coarse_vg = final_state
    attention = stacked[0].reshape(TOKENS, FEAT)
    query_gradient = stacked[1].reshape(TOKENS, FEAT).astype(jnp.bfloat16)
    key_gradient = near_kg[NEAR:] + jnp.repeat(middle_kg[REACH * groups:], MIDG, axis=0) / math.sqrt(MIDG) + jnp.repeat(coarse_kg, FARG, axis=0) / math.sqrt(FARG)
    value_gradient = near_vg[NEAR:] + jnp.repeat(middle_vg[REACH * groups:], MIDG, axis=0) / MIDG + jnp.repeat(coarse_vg, FARG, axis=0) / FARG
    output = jnp.dot(attention, out_weight, preferred_element_type=jnp.float32).astype(jnp.bfloat16)
    weight_grad = jnp.dot(attention.T, out_grad, preferred_element_type=jnp.float32) / math.sqrt(TOKENS)
    return (output, query_gradient, key_gradient.astype(jnp.bfloat16), value_gradient.astype(jnp.bfloat16), weight_grad)
```

```python
import functools
import math

import jax
import jax.numpy as jnp
from jax import lax
from jax.experimental import pallas as pl
from jax.experimental.pallas import tpu as pltpu
from jax.sharding import PartitionSpec as P

HDIM = 64
NEAR = 256
MIDG = 8
FARG = 128
REACH = 12
PAIR = 2 * HDIM
LEVEL = 4
SPAN = REACH // LEVEL + 1
HIDDEN = -1e30


def moved(block, axis, size, target):
    route = [(i, target(i)) for i in range(size) if 0 <= target(i) < size]
    return lax.ppermute(block, axis, route)


def dot(a, b):
    return jnp.dot(a, b, preferred_element_type=jnp.float32)


def prepare_kernel(seq_ref, k_ref, v_ref, pack_ref, rim_ref, *, groups, fars):
    length, features = k_ref.shape
    rows = pack_ref.shape[0]
    level = (seq_ref[0] // LEVEL) % SPAN
    row = lax.broadcasted_iota(jnp.int32, (rows, length), 0)
    col = lax.broadcasted_iota(jnp.int32, (rows, length), 1)
    tail = row - groups
    middle = (row < groups) & (col // MIDG == row)
    coarse = (row >= groups) & (tail // fars == level) & (col // FARG == tail % fars)
    pool = jnp.where(middle | coarse, 1.0, 0.0).astype(jnp.bfloat16)
    is_middle = lax.broadcasted_iota(jnp.int32, (rows, PAIR), 0) < groups
    key_div = jnp.where(is_middle, math.sqrt(MIDG), math.sqrt(FARG))
    value_div = jnp.where(is_middle, float(MIDG), float(FARG))
    for pair in range(features // PAIR):
        lanes = slice(pair * PAIR, (pair + 1) * PAIR)
        base = 2 * pair * PAIR
        key_lanes = slice(base, base + PAIR)
        value_lanes = slice(base + PAIR, base + 2 * PAIR)
        pack_ref[:, key_lanes] = (dot(pool, k_ref[:, lanes]) / key_div).astype(jnp.bfloat16)
        pack_ref[:, value_lanes] = (dot(pool, v_ref[:, lanes]) / value_div).astype(jnp.bfloat16)
        rim_ref[:, key_lanes] = k_ref[length - NEAR :, lanes]
        rim_ref[:, value_lanes] = v_ref[length - NEAR :, lanes]


def attend_kernel(
    seq_ref, keep_ref, frame_ref, q_ref, k_ref, v_ref, mixed_ref, whole_ref, rim_ref, *refs,
    groups, fars, separate,
):
    far_refs = refs[:LEVEL]
    refs = refs[LEVEL:]
    if separate:
        far_coarse_ref = refs[0]
        refs = refs[1:]
    att_ref, dq_ref, near_ref, back_ref, far_ref, weight_ref = refs[:6]
    refs = refs[6:]
    if separate:
        coarse_out_ref = refs[0]
        refs = refs[1:]
    keys, values, keys_t, values_t, bias, score, slope_f, probs, slopes, outs, q_all, g_all = refs
    length = q_ref.shape[0]
    blocks = length // NEAR
    own_end = NEAR + length
    window = REACH * groups
    stride = far_refs[0].shape[0] // SPAN
    total = keys.shape[0]
    far = total - own_end
    coarse = far - window
    pair = pl.program_id(0)
    seq = seq_ref[0]
    spot = seq % LEVEL
    level = seq // LEVEL
    scale = HDIM ** (-0.5)
    to_log2 = scale * math.log2(math.e)

    keys[:NEAR] = rim_ref[:, :PAIR]
    values[:NEAR] = rim_ref[:, PAIR:]
    keys[NEAR:own_end] = k_ref[...]
    values[NEAR:own_end] = v_ref[...]
    places = []
    for slot in range(LEVEL):
        peer = spot ^ slot
        first = jnp.where(peer < spot, 1, 0)
        places.append((peer, first))
        source = far_refs[slot]
        for step in range(SPAN - 1):
            begin = own_end + (slot * (SPAN - 1) + step) * groups
            rows = pl.ds(pl.multiple_of((first + step) * stride, 16), groups)
            keys[begin : begin + groups] = source[rows, :PAIR]
            values[begin : begin + groups] = source[rows, PAIR:]
        if not separate:
            begin = own_end + window + slot * SPAN * fars
            tile = sum(
                source[at * stride + groups : (at + 1) * stride].astype(jnp.float32)
                for at in range(SPAN)
            ).astype(jnp.bfloat16)
            keys[begin : begin + SPAN * fars] = tile[:, :PAIR]
            values[begin : begin + SPAN * fars] = tile[:, PAIR:]
    if separate:
        keys[own_end + window :] = far_coarse_ref[:, :PAIR]
        values[own_end + window :] = far_coarse_ref[:, PAIR:]
    keys_t[...] = keys[...].T
    values_t[...] = values[...].T

    @pl.when(pair == 0)
    def _():
        part = FARG // MIDG
        for block in range(blocks):
            limit = (seq * blocks + block - 1) * NEAR
            for slot in range(LEVEL):
                peer, first = places[slot]
                for step in range(SPAN - 1):
                    at = first + step
                    shard = (level - (SPAN - 1) + at) * LEVEL + peer
                    ahead = at * LEVEL + peer - spot
                    for piece in range(fars):
                        start = shard * length + piece * FARG
                        kept = keep_ref[block, ahead * fars + piece] == 1
                        seen = kept & (shard >= 0) & (start + FARG <= limit)
                        begin = (slot * (SPAN - 1) + step) * groups + piece * part
                        bias[block, begin : begin + part] = jnp.full(
                            (part, PAIR), jnp.where(seen, 0.0, HIDDEN), jnp.float32
                        )
            if separate:
                index = lax.broadcasted_iota(jnp.int32, (coarse, PAIR), 0)
                bias[block, window:] = jnp.where((index + 1) * FARG <= limit, 0.0, HIDDEN)
            else:
                row = lax.broadcasted_iota(jnp.int32, (SPAN * fars, PAIR), 0)
                for slot in range(LEVEL):
                    peer, _ = places[slot]
                    index = ((row // fars) * LEVEL + peer) * fars + row % fars
                    begin = window + slot * SPAN * fars
                    bias[block, begin : begin + SPAN * fars] = jnp.where(
                        (index + 1) * FARG <= limit, 0.0, HIDDEN
                    )

    q_rows = q_ref[...]
    g_rows = mixed_ref[...]
    q_t = q_rows.T
    g_t = g_rows.T
    lane_head = lax.broadcasted_iota(jnp.int32, (NEAR, PAIR), 1) // HDIM
    row_head = lax.broadcasted_iota(jnp.int32, (PAIR, NEAR), 0) // HDIM
    chunk = 128
    for block in range(blocks):
        near_at = block * NEAR
        pieces = [(near_at + c, min(chunk, 2 * NEAR - c)) for c in range(0, 2 * NEAR, chunk)]
        pieces += [(own_end + c, min(chunk, far - c)) for c in range(0, far, chunk)]
        token = slice(near_at, near_at + NEAR)
        open_near = (frame_ref[block] == 1) & (seq * blocks + block > 0)
        near_bias = jnp.where(open_near, 0.0, HIDDEN)
        for head in range(2):
            unit = block * 2 + head
            lanes = slice(unit * NEAR, (unit + 1) * NEAR)
            zero_t = jnp.zeros((PAIR, NEAR), jnp.bfloat16)
            zero = jnp.zeros((NEAR, PAIR), jnp.bfloat16)
            q_head = jnp.where(row_head == head, q_t[:, token], zero_t)
            g_head = jnp.where(row_head == head, g_t[:, token], zero_t)
            q_all[lanes] = jnp.where(lane_head == head, q_rows[token], zero)
            g_all[lanes] = jnp.where(lane_head == head, g_rows[token], zero)
            top = None
            for begin, size in pieces:
                logits = dot(keys[begin : begin + size], q_head) * to_log2
                if begin >= own_end:
                    shade = bias[block, begin - own_end : begin - own_end + size]
                    logits = logits + jnp.concatenate([shade] * (NEAR // PAIR), axis=1)
                elif begin < near_at + NEAR:
                    logits = logits + near_bias
                else:
                    t = lax.broadcasted_iota(jnp.int32, (size, NEAR), 0) + (begin - near_at - NEAR)
                    s = lax.broadcasted_iota(jnp.int32, (size, NEAR), 1)
                    logits = jnp.where(t <= s, logits, HIDDEN)
                score[begin : begin + size] = logits
                high = jnp.max(logits.reshape(-1, 8, NEAR), axis=0)
                top = high if top is None else jnp.maximum(top, high)
            top = jnp.max(top, axis=0, keepdims=True)
            mass = None
            for begin, size in pieces:
                weight = jnp.exp2(score[begin : begin + size] - top)
                score[begin : begin + size] = weight
                part = jnp.sum(weight.reshape(-1, 8, NEAR), axis=0)
                mass = part if mass is None else mass + part
            inverse = 1.0 / jnp.sum(mass, axis=0, keepdims=True)
            centre = None
            for begin, size in pieces:
                rows = slice(begin, begin + size)
                share = score[rows] * inverse
                score[rows] = share
                probs[rows, lanes] = share.astype(jnp.bfloat16)
                gain = dot(values[rows], g_head)
                slope_f[rows] = gain
                part = jnp.sum((share * gain).reshape(-1, 8, NEAR), axis=0)
                centre = part if centre is None else centre + part
            centre = jnp.sum(centre, axis=0, keepdims=True)
            for begin, size in pieces:
                rows = slice(begin, begin + size)
                slopes[rows, lanes] = (score[rows] * (slope_f[rows] - centre)).astype(jnp.bfloat16)
            heads = slice(head * HDIM, (head + 1) * HDIM)
            near = slice(near_at, near_at + 2 * NEAR)
            rest = slice(own_end, total)
            out_t = dot(values_t[heads, near], probs[near, lanes]) + dot(
                values_t[heads, rest], probs[rest, lanes]
            )
            outs[heads, token] = out_t.astype(jnp.bfloat16)
            dq_t = dot(keys_t[heads, near], slopes[near, lanes]) + dot(
                keys_t[heads, rest], slopes[rest, lanes]
            )
            keep = slice(head * HDIM, (head + 1) * HDIM)
            dq_ref[token, keep] = (dq_t * scale).T.astype(jnp.bfloat16)
        att_ref[token] = outs[:, token].T

    def grads(rows, lanes):
        return (
            dot(slopes[rows, lanes], q_all[lanes]) * scale,
            dot(probs[rows, lanes], g_all[lanes]),
        )

    units = 2 * NEAR
    for at in range(blocks + 1):
        low = max(at - 1, 0) * units
        high = min(at + 1, blocks) * units
        key_part, value_part = grads(slice(at * NEAR, (at + 1) * NEAR), slice(low, high))
        if at == 0:
            back_ref[:, :PAIR] = key_part.astype(jnp.bfloat16)
            back_ref[:, PAIR:] = value_part.astype(jnp.bfloat16)
        else:
            near_ref[(at - 1) * NEAR : at * NEAR, :PAIR] = key_part
            near_ref[(at - 1) * NEAR : at * NEAR, PAIR:] = value_part
    every = slice(0, blocks * units)
    for slot in range(LEVEL):
        _, first = places[slot]
        empty = jnp.where(first == 1, 0, SPAN - 1)
        far_ref[slot, pl.ds(pl.multiple_of(empty * stride, 16), groups)] = jnp.zeros(
            (groups, 2 * PAIR), jnp.float32
        )
        begin = own_end + slot * (SPAN - 1) * groups
        key_part, value_part = grads(slice(begin, begin + (SPAN - 1) * groups), every)
        for step in range(SPAN - 1):
            rows = pl.ds(pl.multiple_of((first + step) * stride, 16), groups)
            piece = slice(step * groups, (step + 1) * groups)
            far_ref[slot, rows, :PAIR] = key_part[piece]
            far_ref[slot, rows, PAIR:] = value_part[piece]
    key_part, value_part = grads(slice(own_end + window, total), every)
    if separate:
        coarse_out_ref[:, :PAIR] = key_part
        coarse_out_ref[:, PAIR:] = value_part
    else:
        wide = SPAN * fars
        for slot in range(LEVEL):
            piece = slice(slot * wide, (slot + 1) * wide)
            for at in range(SPAN):
                rows = slice(at * stride + groups, (at + 1) * stride)
                far_ref[slot, rows, :PAIR] = key_part[piece]
                far_ref[slot, rows, PAIR:] = value_part[piece]
    weight = dot(outs[...], whole_ref[...])
    for half in range(PAIR // HDIM):
        slot = (pair * 2 + half) ^ spot
        weight_ref[slot] = weight[half * HDIM : (half + 1) * HDIM]


def combine_kernel(seq_ref, near_ref, back_ref, *refs, groups, fars, separate):
    mid_refs = refs[:SPAN]
    refs = refs[SPAN:]
    if separate:
        coarse_ref = refs[0]
        refs = refs[1:]
    key_ref, value_ref, total = refs
    length = near_ref.shape[0]
    level = (seq_ref[0] // LEVEL) % SPAN
    total[...] = sum(ref[...].astype(jnp.float32) for ref in mid_refs)
    for piece in range(fars):
        if separate:
            far = coarse_ref[piece : piece + 1]
        else:
            far = total[pl.ds(groups + level * fars + piece, 1)]
        key_far = far[:, :PAIR] / math.sqrt(FARG)
        value_far = far[:, PAIR:] / FARG
        for step in range(FARG // MIDG):
            group = piece * (FARG // MIDG) + step
            rows = slice(group * MIDG, (group + 1) * MIDG)
            middle = total[group : group + 1]
            key = near_ref[rows, :PAIR] + (middle[:, :PAIR] / math.sqrt(MIDG) + key_far)
            value = near_ref[rows, PAIR:] + (middle[:, PAIR:] / MIDG + value_far)
            begin = group * MIDG - (length - NEAR)
            if begin >= 0:
                back = back_ref[begin : begin + MIDG].astype(jnp.float32)
                key = key + back[:, :PAIR]
                value = value + back[:, PAIR:]
            key_ref[rows] = key.astype(jnp.bfloat16)
            value_ref[rows] = value.astype(jnp.bfloat16)


def on_device(queries, key_vectors, value_vectors, out_grad, out_weight, mid_keep, frame_keep):
    length, features = queries.shape
    size = lax.axis_size("seq")
    levels = size // LEVEL
    groups = length // MIDG
    fars = length // FARG
    blocks = length // NEAR
    pairs = features // PAIR
    rows = groups + SPAN * fars
    separate = levels > SPAN
    seq = lax.axis_index("seq")
    head = lax.axis_index("head")
    seq_word = seq.astype(jnp.int32).reshape(1)
    bf16 = jnp.bfloat16
    f32 = jnp.float32
    smem = pl.BlockSpec(memory_space=pltpu.SMEM)
    partner = functools.partial(moved, axis="head", size=2, target=lambda i: 1 - i)

    def beside(block, bit):
        return moved(block, "seq", size, lambda i: i ^ bit)

    pack, rim = pl.pallas_call(
        functools.partial(prepare_kernel, groups=groups, fars=fars),
        out_shape=(
            jax.ShapeDtypeStruct((rows, 2 * features), bf16),
            jax.ShapeDtypeStruct((NEAR, 2 * features), bf16),
        ),
        in_specs=[smem, pl.BlockSpec(), pl.BlockSpec()],
        name="prepare",
    )(seq_word, key_vectors, value_vectors)

    rising = [
        moved(pack, "seq", size, lambda i, d=d: i + d * LEVEL) for d in range(SPAN - 1, 0, -1)
    ]
    other_grad = partner(out_grad)
    rim = moved(rim, "seq", size, lambda i: i + 1)
    half = out_weight.shape[1] // 2
    mine = lax.dynamic_slice_in_dim(out_weight, head * half, half, 1)
    theirs = lax.dynamic_slice_in_dim(out_weight, (1 - head) * half, half, 1)
    other_weight = partner(theirs)
    column = jnp.concatenate(rising + [pack], axis=0)
    across = beside(column, 2)
    inner = beside(column, 1)
    corner = beside(across, 1)
    contract = (((1,), (1,)), ((), ()))
    mixed = (
        lax.dot_general(out_grad, mine, contract, preferred_element_type=f32)
        + lax.dot_general(other_grad, theirs, contract, preferred_element_type=f32)
    ).astype(bf16)
    whole = jnp.where(
        head == 0,
        jnp.concatenate([out_grad, other_grad], axis=1),
        jnp.concatenate([other_grad, out_grad], axis=1),
    )
    far_inputs = [column, inner, across, corner]
    coarse_count = size * fars if separate else LEVEL * SPAN * fars
    if separate:
        slim = lax.dynamic_slice_in_dim(pack, groups + (seq // LEVEL % SPAN) * fars, fars, 0)
        far_inputs.append(lax.all_gather(slim, "seq", axis=0, tiled=True))
    total = NEAR + length + REACH * groups + coarse_count
    units = 2 * blocks * NEAR
    by_pair = lambda n, width: pl.BlockSpec((n, width), lambda p: (0, p))
    out_shape = [
        jax.ShapeDtypeStruct((length, features), bf16),
        jax.ShapeDtypeStruct((length, features), bf16),
        jax.ShapeDtypeStruct((length, 2 * features), f32),
        jax.ShapeDtypeStruct((NEAR, 2 * features), bf16),
        jax.ShapeDtypeStruct((LEVEL, SPAN * rows, 2 * features), f32),
        jax.ShapeDtypeStruct((LEVEL, features // LEVEL, 2 * half), f32),
    ]
    out_specs = [
        by_pair(length, PAIR),
        by_pair(length, PAIR),
        by_pair(length, 2 * PAIR),
        by_pair(NEAR, 2 * PAIR),
        pl.BlockSpec((LEVEL, SPAN * rows, 2 * PAIR), lambda p: (0, 0, p)),
        pl.BlockSpec((LEVEL, features // LEVEL, 2 * half), lambda p: (0, 0, 0)),
    ]
    if separate:
        out_shape.append(jax.ShapeDtypeStruct((coarse_count, 2 * features), f32))
        out_specs.append(by_pair(coarse_count, 2 * PAIR))
    results = pl.pallas_call(
        functools.partial(attend_kernel, groups=groups, fars=fars, separate=separate),
        grid=(pairs,),
        out_shape=out_shape,
        in_specs=[smem, smem, smem]
        + [by_pair(length, PAIR)] * 4
        + [pl.BlockSpec((length, 2 * half), lambda p: (0, 0)), by_pair(NEAR, 2 * PAIR)]
        + [by_pair(item.shape[0], 2 * PAIR) for item in far_inputs],
        out_specs=out_specs,
        scratch_shapes=[
            pltpu.VMEM((total, PAIR), bf16),
            pltpu.VMEM((total, PAIR), bf16),
            pltpu.VMEM((PAIR, total), bf16),
            pltpu.VMEM((PAIR, total), bf16),
            pltpu.VMEM((blocks, REACH * groups + coarse_count, PAIR), f32),
            pltpu.VMEM((total, NEAR), f32),
            pltpu.VMEM((total, NEAR), f32),
            pltpu.VMEM((total, units), bf16),
            pltpu.VMEM((total, units), bf16),
            pltpu.VMEM((PAIR, length), bf16),
            pltpu.VMEM((units, PAIR), bf16),
            pltpu.VMEM((units, PAIR), bf16),
        ],
        compiler_params=pltpu.CompilerParams(dimension_semantics=("arbitrary",)),
        name="attend",
    )(seq_word, mid_keep, frame_keep, queries, key_vectors, value_vectors, mixed, whole, rim,
      *far_inputs)
    attention, query_gradient, near, back, far, weight = results[:6]

    other_attention = partner(attention)
    sides = [
        (far[2 * at] + beside(far[2 * at + 1], 1), weight[2 * at] + beside(weight[2 * at + 1], 1))
        for at in (1, 0)
    ]
    sent = [part.astype(bf16) for part in sides[0]]
    far_sum = sides[1][0] + beside(sent[0], 2).astype(f32)
    weight_sum = sides[1][1] + beside(sent[1], 2).astype(f32)
    back = moved(back, "seq", size, lambda i: i - 1)
    stages = [far_sum[at * rows : (at + 1) * rows].astype(bf16) for at in range(SPAN)]
    pieces = [
        moved(stages[at], "seq", size, lambda i, d=SPAN - 1 - at: i - d * LEVEL)
        for at in range(SPAN - 1)
    ]
    pieces.append(far_sum[(SPAN - 1) * rows :])
    if separate:
        pieces.append(lax.psum_scatter(results[6], "seq", scatter_dimension=0, tiled=True))

    root = math.sqrt(length * size)
    if separate:
        order = [(seq % LEVEL) ^ slot for slot in range(LEVEL)]
        flat = jnp.concatenate(
            [lax.dynamic_index_in_dim(weight, at ^ (seq % LEVEL), 0, False) for at in range(LEVEL)]
        )
        weight_grad = lax.psum(flat, "seq") / root
    else:
        narrow = weight_sum.astype(bf16)
        for distance in range(1, levels):
            weight_sum = weight_sum + moved(
                narrow, "seq", size, lambda i, d=distance: (i + d * LEVEL) % size
            ).astype(f32)
        weight_sum = weight_sum / root
        weight_across = beside(weight_sum, 2)
        tiles = [
            weight_sum, beside(weight_sum, 1), weight_across, beside(weight_across, 1)
        ]
        stack = jnp.stack(tiles)
        weight_grad = jnp.concatenate(
            [lax.dynamic_index_in_dim(stack, at ^ (seq % LEVEL), 0, False) for at in range(LEVEL)]
        )

    key_gradient, value_gradient = pl.pallas_call(
        functools.partial(combine_kernel, groups=groups, fars=fars, separate=separate),
        grid=(pairs,),
        out_shape=(
            jax.ShapeDtypeStruct((length, features), bf16),
            jax.ShapeDtypeStruct((length, features), bf16),
        ),
        in_specs=[smem, by_pair(length, 2 * PAIR), by_pair(NEAR, 2 * PAIR)]
        + [by_pair(piece.shape[0], 2 * PAIR) for piece in pieces],
        out_specs=(by_pair(length, PAIR), by_pair(length, PAIR)),
        scratch_shapes=[pltpu.VMEM((rows, 2 * PAIR), f32)],
        name="combine",
    )(seq_word, near, back, *pieces)
    output = (dot(attention, mine) + dot(other_attention, other_weight)).astype(bf16)
    return output, query_gradient, key_gradient, value_gradient, weight_grad


def solution(mesh):
    in_specs = (
        P("seq", "head"),
        P("seq", "head"),
        P("seq", "head"),
        P("seq", "head"),
        P("head", None),
        P("seq", None),
        P("seq"),
    )
    out_specs = (
        P("seq", "head"),
        P("seq", "head"),
        P("seq", "head"),
        P("seq", "head"),
        P("head", None),
    )
    return jax.shard_map(
        on_device, mesh=mesh, in_specs=in_specs, out_specs=out_specs, check_vma=False
    )
```
